32 devices in a mesh: section: 2 (over x), dp: 4 (over z), mp: 4 (over y, core).
Axes of the slice: x: 2, y: 2, z: 4, core: 2. Of those that a mesh axis runs over, the one named last changes fastest.
Arguments:
- text_feats: bfloat16 [4096, 512], P('dp'), may hold values from -48 to 48
- image_feats: bfloat16 [4096, 512], P(('dp', 'mp')), may hold values from -48 to 48
- logit_scale: float32 [1], replicated, may hold values from 10 to 320
- layer_inputs: bfloat16 [2, 4096, 512], P('section', 'dp'), may hold values from -6 to 6
- w_in: bfloat16 [2, 512, 2048], P('section', None, 'mp'), may hold values from -0.25 to 0.25
- w_out: bfloat16 [2, 2048, 512], P('section', 'mp'), may hold values from -0.125 to 0.125
Outputs:
- image_grad: bfloat16 [4096, 512], P(('dp', 'mp'))
- input_grad: bfloat16 [4096, 512], P('dp', 'section')
- w_in_grad: float32 [2, 512, 2048], P('section', 'dp', 'mp')
- w_out_grad_t: float32 [2, 512, 2048], P('section', 'dp', 'mp')
The draws below stay inside these ranges and needn't reach their ends.
All inputs are finite; a program needn't handle non-finite values.
Results may differ from the reference program's by a relative error of at most 0.017.
Values may be sent and summed in bfloat16 or wider, within the bound.
A program may use at most 128 MiB of HBM per device.

```python
import jax
import jax.numpy as jnp
from jax import lax

D = 512
FF = 2048
PAIRS_DEV = 1024
PAIRS = 4096
LAYERS = 2


def joint_feats(key):
    folded = jax.random.fold_in(key, 11)
    key_shared, key_text, key_image, key_scale = jax.random.split(folded, 4)
    shared = jnp.clip(jax.random.normal(key_shared, (PAIRS, D), jnp.float32), -4.0, 4.0)
    text_noise = jnp.clip(jax.random.normal(key_text, (PAIRS, D), jnp.float32), -4.0, 4.0)
    image_noise = jnp.clip(jax.random.normal(key_image, (PAIRS, D), jnp.float32), -4.0, 4.0)
    text_rows = shared + text_noise
    image_rows = shared + image_noise
    return (text_rows, image_rows)


def draw_text_feats(key, part):
    text_rows, image_rows = joint_feats(key)
    return text_rows.astype(jnp.bfloat16)


def draw_image_feats(key, part):
    text_rows, image_rows = joint_feats(key)
    return image_rows.astype(jnp.bfloat16)


def draw_logit_scale(key, part):
    folded = jax.random.fold_in(key, 23)
    return jax.random.uniform(folded, (1,), jnp.float32, 10.0, 30.0)


def block_levels(rng, dims, cuts, smallest, top_value):
    factor_of, own = 1.0, jax.random.fold_in(rng, 6)
    for dim, parts in cuts:
        steps = jnp.exp(jax.random.uniform(jax.random.fold_in(own, dim), (parts,), jnp.float32, smallest / len(cuts), top_value / len(cuts)))
        factor_of = factor_of * jnp.repeat(steps, dims[dim] // parts).reshape([-1 if axis == dim else 1 for axis in range(len(dims))])
    return factor_of


def gaussian(key, extent, deviation, limit, cuts=(), kind=jnp.bfloat16):
    entries = jax.random.normal(key, extent, jnp.float32) * deviation
    if len(cuts) > 0:
        entries = block_levels(key, extent, cuts, -0.22, 0.18) * entries
    return jnp.clip(entries, min=-limit, max=limit).astype(kind)


def setup_inputs(seed: int = 0) -> dict:
    splits = jax.random.split(jax.random.key(seed), 7)
    text_feats = draw_text_feats(jax.random.fold_in(splits[6], 71), 0)
    image_feats = draw_image_feats(jax.random.fold_in(splits[6], 71), 0)
    logit_scale = draw_logit_scale(jax.random.fold_in(splits[6], 71), 0)
    layer_inputs = gaussian(splits[3], (LAYERS, PAIRS, D), 1.0, 6.0, ((0, 2), (1, 4)))
    w_in = gaussian(splits[4], (LAYERS, D, FF), D ** -0.5, 0.25, ((0, 2), (2, 4)))
    w_out = gaussian(splits[5], (LAYERS, FF, D), FF ** -0.5, 0.125, ((0, 2), (1, 4)))
    return {"text_feats": text_feats, "image_feats": image_feats, "logit_scale": logit_scale, "layer_inputs": layer_inputs, "w_in": w_in, "w_out": w_out}


def unit_rows(values):
    wide = values.astype(jnp.float32)
    length = jnp.sqrt(lax.optimization_barrier(jnp.sum(wide * wide, axis=1, keepdims=True)) + 1.0)
    return (wide / length, length)

def unit_backward(unit, length, grad_unit):
    return (grad_unit - unit * lax.optimization_barrier(jnp.sum(unit * grad_unit, axis=1, keepdims=True))) / length

def quick_gelu(values):
    return values * jax.nn.sigmoid(1.702 * values)

def quick_slope(values):
    sigm = jax.nn.sigmoid(1.702 * values)
    return sigm + 1.702 * values * sigm * (1.0 - sigm)

def reference(text_feats, image_feats, logit_scale, layer_inputs, w_in, w_out):
    logit_mult = logit_scale[0]
    text_unit, text_length = unit_rows(text_feats)
    image_unit, image_length = unit_rows(image_feats)
    text_low = text_unit.astype(jnp.bfloat16)
    image_low = image_unit.astype(jnp.bfloat16)
    block_count = PAIRS // PAIRS_DEV
    text_blocks = text_low.reshape(block_count, PAIRS_DEV, D)
    block_ids = jnp.arange(block_count, dtype=jnp.int32)
    column_ids = jnp.arange(PAIRS, dtype=jnp.int32)

    def stats_step(state_pair, text_block):
        column_peak, column_total = state_pair
        scores = logit_mult * jnp.dot(text_block, image_low.T, preferred_element_type=jnp.float32)
        row_peak = lax.optimization_barrier(jnp.max(scores, axis=1))
        row_total = lax.optimization_barrier(jnp.sum(jnp.exp(scores - row_peak[:, None]), axis=1))
        new_peak = jnp.maximum(column_peak, lax.optimization_barrier(jnp.max(scores, axis=0)))
        column_total = column_total * jnp.exp(column_peak - new_peak) + lax.optimization_barrier(jnp.sum(jnp.exp(scores - new_peak[None, :]), axis=0))
        return ((new_peak, column_total), (row_peak, row_total))
    start_pair = (jnp.full((PAIRS,), -1e+30, jnp.float32), jnp.zeros((PAIRS,), jnp.float32))
    (column_peak, column_total), (row_peaks, row_totals) = lax.scan(stats_step, start_pair, text_blocks)

    def grad_step(image_acc, inputs):
        text_block, row_peak, row_total, block_id = inputs
        scores = logit_mult * jnp.dot(text_block, image_low.T, preferred_element_type=jnp.float32)
        text_ids = (block_id * PAIRS_DEV + jnp.arange(PAIRS_DEV, dtype=jnp.int32)).astype(jnp.int32)
        positive = (text_ids[:, None] == column_ids[None, :]).astype(jnp.float32)
        row_prob = jnp.exp(scores - row_peak[:, None]) / row_total[:, None]
        column_prob = jnp.exp(scores - column_peak[None, :]) / column_total[None, :]
        score_grad = (0.5 * (row_prob + column_prob) - positive).astype(jnp.bfloat16)
        text_part = logit_mult * jnp.dot(score_grad, image_low, preferred_element_type=jnp.float32)
        image_acc = image_acc + logit_mult * jnp.dot(score_grad.T, text_block, preferred_element_type=jnp.float32)
        return (image_acc, text_part)
    image_unit_grad, text_parts = lax.scan(grad_step, jnp.zeros((PAIRS, D), jnp.float32), (text_blocks, row_peaks, row_totals, block_ids))
    text_unit_grad = text_parts.reshape(PAIRS, D)
    top_grad = unit_backward(text_unit, text_length, text_unit_grad).astype(jnp.bfloat16)
    image_grad = unit_backward(image_unit, image_length, image_unit_grad).astype(jnp.bfloat16)
    layer_grad = top_grad
    first_grads = []
    second_grads = []
    for layer in reversed(range(LAYERS)):
        inputs_now = layer_inputs[layer]
        pre_act = jnp.dot(inputs_now, w_in[layer], preferred_element_type=jnp.float32)
        activation = quick_gelu(pre_act).astype(jnp.bfloat16)
        back_grad = jnp.dot(layer_grad, w_out[layer].T, preferred_element_type=jnp.float32)
        pre_grad = (back_grad * quick_slope(pre_act)).astype(jnp.bfloat16)
        first_grads.insert(0, jnp.dot(inputs_now.T, pre_grad, preferred_element_type=jnp.float32))
        second_grads.insert(0, jnp.dot(layer_grad.T, activation, preferred_element_type=jnp.float32))
        layer_grad = (layer_grad.astype(jnp.float32) + jnp.dot(pre_grad, w_in[layer].T, preferred_element_type=jnp.float32)).astype(jnp.bfloat16)
    return (image_grad, layer_grad, jnp.stack(first_grads), jnp.stack(second_grads))
```

```python
import jax
import jax.numpy as jnp
from jax import lax
from jax.experimental import pallas as pl
from jax.experimental.pallas import tpu as pltpu
from jax.sharding import PartitionSpec as P

MESH = pl.DeviceIdType.MESH
F32 = jnp.float32
BF16 = jnp.bfloat16
GELU = 1.702
LANES = 128


def unit_rows(values):
    wide = values.astype(F32)
    length = jnp.sqrt(jnp.sum(wide * wide, axis=1, keepdims=True) + 1.0)
    return (wide / length, length)


def unit_backward(unit, length, grad_unit):
    return (grad_unit - unit * jnp.sum(unit * grad_unit, axis=1, keepdims=True)) / length


def dot_nn(a, b):
    return lax.dot_general(a, b, (((1,), (0,)), ((), ())), preferred_element_type=F32)


def dot_nt(a, b):
    return lax.dot_general(a, b, (((1,), (1,)), ((), ())), preferred_element_type=F32)


def dot_tn(a, b):
    return lax.dot_general(a, b, (((0,), (0,)), ((), ())), preferred_element_type=F32)


def tile(index, size):
    return pl.ds(pl.multiple_of(index * size, size), size)


def make_kernel(n_sec, n_dp, n_mp):
    cores = 2 if n_mp % 2 == 0 else 1
    chips = n_mp // cores

    def kernel(
        text, image, scale_ref, hidden, w_in, w_out,
        image_out, input_out, first_out, second_out,
        text_low, cols, scores, sgrad, row_max, row_lse, row_st, row_rx, col_st, col_rx,
        wi_all, wo_all, t_tx, t_rx, t_own, g_all, g_acc, g_new, act_all, pre_all,
        w_tx, w_rx, i_tx, i_rx,
        gat_s, gat_r, fwd_s, fwd_r, cs_s, cs_r, rs_s, rs_r, wi_s, wi_r, wo_s, wo_r,
        t_s, t_r, g_s, g_r, x_s, x_r, in_s, in_r, ix_s, ix_r, w_s, w_r, im_s, im_r, io_s, io_r,
    ):
        s = lax.axis_index("section")
        d = lax.axis_index("dp")
        m = lax.axis_index("mp")
        last = n_sec - 1
        rows = text.shape[0]
        own = image.shape[0]
        half = own // n_sec
        quarter = rows // n_mp
        feats = text.shape[1]
        share = feats // n_dp
        width = feats // n_sec
        mult = scale_ref[0]
        core = lax.rem(m, cores)
        chip = m // cores

        def copy(src, dst, send, recv, where):
            return pltpu.make_async_remote_copy(
                src_ref=src, dst_ref=dst, send_sem=send, recv_sem=recv,
                device_id=where, device_id_type=MESH,
            )

        def others(mine, count):
            return [lax.rem(mine + k, count) for k in range(1, count)]

        def sources(mine, count):
            return [lax.rem(mine + count - k, count) for k in range(1, count)]

        barrier = pltpu.get_barrier_semaphore()
        for p in others(d, n_dp):
            pl.semaphore_signal(barrier, inc=1, device_id={"dp": p}, device_id_type=MESH)
        for p in others(m, n_mp):
            pl.semaphore_signal(barrier, inc=1, device_id={"mp": p}, device_id_type=MESH)
        for p in others(s, n_sec):
            pl.semaphore_signal(barrier, inc=1, device_id={"section": p}, device_id_type=MESH)

        own_unit, _ = unit_rows(image[...])
        cols[tile(d, own), :] = own_unit.astype(BF16)
        pl.semaphore_wait(barrier, n_dp + n_mp + n_sec - 3)

        def cut(block, sec):
            return cols.at[pl.ds(pl.multiple_of(block * own + sec * half, half), half), :]

        gathers = []
        for p in others(d, n_dp):
            c = copy(cut(d, s), cut(d, s), gat_s.at[p], gat_r.at[d], {"dp": p})
            c.start()
            gathers.append(c)

        class Spread:
            def __init__(self, slot, send, recv):
                self.slot, self.send, self.recv = slot, send, recv
                self.sent = []

            def push(self, index, to):
                c = copy(self.slot(index), self.slot(index), self.send.at[len(self.sent)],
                         self.recv.at[index], {"mp": to})
                c.start()
                self.sent.append(c)

            def arrived(self, index):
                copy(self.slot(index), self.slot(index), self.send.at[0],
                     self.recv.at[index], {"mp": lax.rem(m + 1, n_mp)}).wait_recv()

            def start(self):
                for q in others(chip, chips):
                    self.push(m, q * cores + core)
                for e in others(core, cores):
                    self.push(m, chip * cores + e)

            def relay(self):
                for q in sources(chip, chips):
                    index = q * cores + core
                    self.arrived(index)
                    for e in others(core, cores):
                        self.push(index, chip * cores + e)

            def finish(self):
                for e in sources(core, cores):
                    self.arrived(chip * cores + e)
                    for q in sources(chip, chips):
                        self.arrived(q * cores + e)

            def drain(self):
                for c in self.sent:
                    c.wait_send()

        wi_all[m] = w_in[...]
        wo_all[m] = w_out[...]
        wi_spread = Spread(lambda k: wi_all.at[k], wi_s, wi_r)
        wo_spread = Spread(lambda k: wo_all.at[k], wo_s, wo_r)
        wi_spread.start()
        wo_spread.start()

        @pl.loop(0, n_mp)
        def _(r):
            unit, _ = unit_rows(text[tile(r, quarter), :])
            text_low[tile(r, quarter), :] = unit.astype(BF16)

        row_max[...] = jnp.full(row_max.shape, -1e30, F32)

        def block_scores(p):
            piece = cols[tile(p, own), :]

            def chunk(r, peak):
                value = mult * dot_nt(text_low[tile(r, quarter), :], piece)
                scores[tile(r, quarter), tile(p, own)] = value
                best = row_max[tile(r, quarter), :]
                for k in range(0, own, LANES):
                    best = jnp.maximum(best, value[:, k : k + LANES])
                row_max[tile(r, quarter), :] = best
                return jnp.maximum(peak, jnp.max(value, axis=0, keepdims=True))

            peak = lax.fori_loop(0, n_mp, chunk, jnp.full((1, own), -1e30, F32))

            def total(r, acc):
                value = scores[tile(r, quarter), tile(p, own)]
                return acc + jnp.sum(jnp.exp(value - peak), axis=0, keepdims=True)

            acc = lax.fori_loop(0, n_mp, total, jnp.zeros((1, own), F32))
            col_st[pl.ds(p, 1), :] = peak
            col_st[pl.ds(n_dp + p, 1), :] = acc

        block_scores(d)
        forwards = []
        for k, p in enumerate(sources(d, n_dp)):
            copy(cut(p, s), cut(p, s), gat_s.at[p], gat_r.at[p], {"dp": p}).wait_recv()
            for t in others(s, n_sec):
                c = copy(cut(p, s), cut(p, s), fwd_s.at[t, p], fwd_r.at[s, p], {"section": t})
                c.start()
                forwards.append(c)
        for p in sources(d, n_dp):
            for t in sources(s, n_sec):
                copy(cut(p, t), cut(p, t), fwd_s.at[t, p], fwd_r.at[t, p],
                     {"section": t}).wait_recv()
            block_scores(p)

        col_rx[d] = col_st[...]
        col_sent = []
        for p in others(d, n_dp):
            c = copy(col_st, col_rx.at[d], cs_s.at[p], cs_r.at[d], {"dp": p})
            c.start()
            col_sent.append(c)

        for r in range(n_mp):
            part = pl.ds(r * quarter, quarter)
            peak = jnp.max(row_max[part, :], axis=1, keepdims=True)

            def total(p, acc):
                value = jnp.exp(scores[part, tile(p, own)] - peak)
                for k in range(0, own, LANES):
                    acc = acc + value[:, k : k + LANES]
                return acc

            acc = lax.fori_loop(0, n_dp, total, jnp.zeros((quarter, LANES), F32))
            acc = jnp.sum(acc, axis=1, keepdims=True)
            wide_peak = jnp.broadcast_to(peak, (quarter, LANES)).T
            wide_sum = jnp.broadcast_to(acc, (quarter, LANES)).T
            row_st[r : r + 1, :] = wide_peak[0:1, :]
            row_st[n_mp + r : n_mp + r + 1, :] = wide_sum[0:1, :]

        row_rx[m] = row_st[...]
        row_sent = []
        for p in others(m, n_mp):
            c = copy(row_st, row_rx.at[m], rs_s.at[p], rs_r.at[m], {"mp": p})
            c.start()
            row_sent.append(c)

        def merge(rx, count, n):
            peak = rx[0, 0:n, :]
            for k in range(1, count):
                peak = jnp.maximum(peak, rx[k, 0:n, :])
            acc = jnp.zeros(peak.shape, F32)
            for k in range(count):
                acc = acc + rx[k, n : 2 * n, :] * jnp.exp(rx[k, 0:n, :] - peak)
            return peak + jnp.log(acc)

        for p in sources(d, n_dp):
            copy(col_st, col_rx.at[p], cs_s.at[p], cs_r.at[p], {"dp": p}).wait_recv()
        col_lse = merge(col_rx, n_dp, n_dp)
        col_st_rows = [col_lse[k : k + 1, :] for k in range(n_dp)]
        for p in sources(m, n_mp):
            copy(row_st, row_rx.at[p], rs_s.at[p], rs_r.at[p], {"mp": p}).wait_recv()
        merged = merge(row_rx, n_mp, n_mp)
        for r in range(n_mp):
            row_lse[r] = jnp.broadcast_to(merged[r : r + 1, :], (LANES, quarter)).T

        def score_rows(r):
            line = row_lse[r]
            text_id = lax.broadcasted_iota(jnp.int32, (quarter, LANES), 0) + d * rows + r * quarter
            for p in range(n_dp):
                for k in range(0, own, LANES):
                    value = scores[tile(r, quarter), p * own + k : p * own + k + LANES]
                    both = jnp.exp(value - line) + jnp.exp(value - col_st_rows[p][:, k : k + LANES])
                    image_id = lax.broadcasted_iota(jnp.int32, (quarter, LANES), 1) + (
                        (p * n_mp + m) * own + k
                    )
                    out = 0.5 * both - jnp.where(text_id == image_id, 1.0, 0.0)
                    sgrad[tile(r, quarter), p * own + k : p * own + k + LANES] = out.astype(BF16)

        @pl.loop(0, n_mp)
        def _(k):
            r = lax.rem(m + 1 + k, n_mp)
            score_rows(r)

            @pl.when(s == last)
            def _():
                value = dot_nn(sgrad[tile(r, quarter), :], cols[...])

                @pl.when(k < n_mp - 1)
                def _():
                    t_tx[r] = value.astype(BF16)
                    copy(t_tx.at[r], t_rx.at[m], t_s.at[r], t_r.at[m], {"mp": r}).start()

                @pl.when(k == n_mp - 1)
                def _():
                    t_own[...] = value

        def image_part(p):
            at = pl.ds(pl.multiple_of(p * own + s * half, half), half)
            return dot_tn(sgrad[:, at], text_low[...])

        image_sent = []
        for p in others(d, n_dp):
            i_tx[p] = image_part(p).astype(BF16)
            c = copy(i_tx.at[p], i_rx.at[d], im_s.at[p], im_r.at[d], {"dp": p})
            c.start()
            image_sent.append(c)

        wi_spread.relay()
        wo_spread.relay()

        mine = tile(m, quarter)

        @pl.when(s == last)
        def _():
            total = t_own[...]
            for p in sources(m, n_mp):
                copy(t_tx.at[p], t_rx.at[p], t_s.at[p], t_r.at[p], {"mp": p}).wait_recv()
                total = total + t_rx[p].astype(F32)
            unit, length = unit_rows(text[mine, :])
            g_all[m] = unit_backward(unit, length, mult * total).astype(BF16)

        wi_spread.finish()
        wo_spread.finish()

        @pl.when(s != last)
        def _():
            copy(g_new, g_all.at[m], x_s, x_r, {"section": s + 1}).wait_recv()

        g_spread = Spread(lambda k: g_all.at[k], g_s, g_r)
        g_spread.start()

        def slopes(pre, back):
            sigm = 1.0 / (1.0 + jnp.exp(-GELU * pre))
            grad = back * (sigm + GELU * pre * sigm * (1.0 - sigm))
            return (pre * sigm).astype(BF16), grad.astype(BF16)

        g_acc[...] = g_all[m].astype(F32)

        @pl.loop(0, n_mp)
        def _(j):
            pre = dot_nn(hidden[mine, :], wi_all[j])
            back = dot_nt(g_all[m], wo_all[j])
            _, grad = slopes(pre, back)
            g_acc[...] += dot_nt(grad, wi_all[j])

        g_new[...] = g_acc[...].astype(BF16)

        @pl.when(s > 0)
        def _():
            copy(g_new, g_all.at[m], x_s, x_r, {"section": s - 1}).start()

        def slab(k):
            return input_out.at[tile(k, quarter), :]

        def final(t):
            return copy(g_new.at[:, t * width : (t + 1) * width], slab(m), ix_s.at[t], ix_r,
                        {"section": t})

        @pl.when(s == 0)
        def _():
            for t in range(1, n_sec):
                final(t).start()
            input_out[mine, :] = g_new[:, 0:width]

        g_spread.relay()
        g_spread.finish()
        in_spread = Spread(slab, in_s, in_r)

        @pl.loop(0, n_mp)
        def _(r):
            pre = dot_nn(hidden[tile(r, quarter), :], w_in[...])
            back = dot_nt(g_all[r], w_out[...])
            act, grad = slopes(pre, back)
            act_all[tile(r, quarter), :] = act
            pre_all[tile(r, quarter), :] = grad

        g_rows = g_all[...].reshape(rows, feats)
        grad_second = dot_tn(g_rows, act_all[...])
        for p in range(n_dp):
            w_tx[p, 1] = grad_second[p * share : (p + 1) * share, :].astype(BF16)
        weight_sent = []

        def send_weights(which):
            for p in others(d, n_dp):
                c = copy(w_tx.at[p, which], w_rx.at[d, which], w_s.at[which, p],
                         w_r.at[which, d], {"dp": p})
                c.start()
                weight_sent.append(c)

        send_weights(1)
        grad_first = dot_tn(hidden[...], pre_all[...])
        for p in range(n_dp):
            w_tx[p, 0] = grad_first[p * share : (p + 1) * share, :].astype(BF16)
        send_weights(0)

        @pl.when(s != 0)
        def _():
            copy(g_new.at[:, 0:width], slab(m), ix_s.at[0], ix_r, {"section": 0}).wait_recv()

        in_spread.start()

        image_half = pl.ds(pl.multiple_of(s * half, half), half)
        total = image_part(d)
        for p in sources(d, n_dp):
            copy(i_tx.at[p], i_rx.at[p], im_s.at[p], im_r.at[p], {"dp": p}).wait_recv()
            total = total + i_rx[p].astype(F32)
        unit, length = unit_rows(image[image_half, :])
        image_out[image_half, :] = unit_backward(unit, length, mult * total).astype(BF16)
        out_sent = []
        for t in others(s, n_sec):
            c = copy(image_out.at[image_half, :], image_out.at[image_half, :],
                     io_s.at[t], io_r.at[s], {"section": t})
            c.start()
            out_sent.append(c)

        in_spread.relay()
        in_spread.finish()

        for which, out in ((1, second_out), (0, first_out)):
            total = w_tx[d, which].astype(F32)
            for p in sources(d, n_dp):
                copy(w_tx.at[p, which], w_rx.at[p, which], w_s.at[which, p],
                     w_r.at[which, p], {"dp": p}).wait_recv()
                total = total + w_rx[p, which].astype(F32)
            out[...] = total

        for t in sources(s, n_sec):
            part = image_out.at[pl.ds(pl.multiple_of(t * half, half), half), :]
            copy(part, part, io_s.at[t], io_r.at[t], {"section": t}).wait_recv()

        for c in gathers + forwards + col_sent + row_sent + image_sent + weight_sent + out_sent:
            c.wait_send()
        for spread in (wi_spread, wo_spread, g_spread, in_spread):
            spread.drain()

        @pl.when(s == last)
        def _():
            for p in others(m, n_mp):
                copy(t_tx.at[p], t_rx.at[m], t_s.at[p], t_r.at[m], {"mp": p}).wait_send()

        @pl.when(s > 0)
        def _():
            copy(g_new, g_all.at[m], x_s, x_r, {"section": s - 1}).wait_send()

        @pl.when(s == 0)
        def _():
            for t in range(1, n_sec):
                final(t).wait_send()

    return kernel


def solution(mesh):
    n_sec, n_dp, n_mp = mesh.shape["section"], mesh.shape["dp"], mesh.shape["mp"]

    def body(text, image, scale, hidden, w_in, w_out):
        rows, feats = text.shape
        own = image.shape[0]
        hid = w_in.shape[2]
        quarter, half, share = rows // n_mp, own // n_sec, feats // n_dp
        columns = own * n_dp
        dma = pltpu.SemaphoreType.DMA
        vmem = pl.BlockSpec(memory_space=pltpu.VMEM)
        out = pl.pallas_call(
            make_kernel(n_sec, n_dp, n_mp),
            out_shape=(
                jax.ShapeDtypeStruct((own, feats), BF16),
                jax.ShapeDtypeStruct((rows, feats // n_sec), BF16),
                jax.ShapeDtypeStruct((share, hid), F32),
                jax.ShapeDtypeStruct((share, hid), F32),
            ),
            in_specs=[vmem, vmem, pl.BlockSpec(memory_space=pltpu.SMEM), vmem, vmem, vmem],
            out_specs=(vmem,) * 4,
            scratch_shapes=[
                pltpu.VMEM((rows, feats), BF16),
                pltpu.VMEM((columns, feats), BF16),
                pltpu.VMEM((rows, columns), F32),
                pltpu.VMEM((rows, columns), BF16),
                pltpu.VMEM((rows, LANES), F32),
                pltpu.VMEM((n_mp, quarter, LANES), F32),
                pltpu.VMEM((2 * n_mp, quarter), F32),
                pltpu.VMEM((n_mp, 2 * n_mp, quarter), F32),
                pltpu.VMEM((2 * n_dp, own), F32),
                pltpu.VMEM((n_dp, 2 * n_dp, own), F32),
                pltpu.VMEM((n_mp, feats, hid), BF16),
                pltpu.VMEM((n_mp, hid, feats), BF16),
                pltpu.VMEM((n_mp, quarter, feats), BF16),
                pltpu.VMEM((n_mp, quarter, feats), BF16),
                pltpu.VMEM((quarter, feats), F32),
                pltpu.VMEM((n_mp, quarter, feats), BF16),
                pltpu.VMEM((quarter, feats), F32),
                pltpu.VMEM((quarter, feats), BF16),
                pltpu.VMEM((rows, hid), BF16),
                pltpu.VMEM((rows, hid), BF16),
                pltpu.VMEM((n_dp, 2, share, hid), BF16),
                pltpu.VMEM((n_dp, 2, share, hid), BF16),
                pltpu.VMEM((n_dp, half, feats), BF16),
                pltpu.VMEM((n_dp, half, feats), BF16),
                dma((n_dp,)), dma((n_dp,)),
                dma((n_sec, n_dp)), dma((n_sec, n_dp)),
                dma((n_dp,)), dma((n_dp,)),
                dma((n_mp,)), dma((n_mp,)),
                dma((2 * n_mp,)), dma((n_mp,)),
                dma((2 * n_mp,)), dma((n_mp,)),
                dma((n_mp,)), dma((n_mp,)),
                dma((2 * n_mp,)), dma((n_mp,)),
                dma, dma,
                dma((2 * n_mp,)), dma((n_mp,)),
                dma((n_sec,)), dma,
                dma((2, n_dp)), dma((2, n_dp)),
                dma((n_dp,)), dma((n_dp,)),
                dma((n_sec,)), dma((n_sec,)),
            ],
            compiler_params=pltpu.CompilerParams(
                collective_id=0, has_side_effects=True, vmem_limit_bytes=63000000
            ),
        )(text, image, scale, hidden[0], w_in[0], w_out[0])
        image_grad, input_grad, first, second = out
        return (image_grad, input_grad, first[None], second[None])

    return jax.shard_map(
        body,
        mesh=mesh,
        in_specs=(
            P("dp", None),
            P(("dp", "mp"), None),
            P(),
            P("section", "dp", None),
            P("section", None, "mp"),
            P("section", "mp", None),
        ),
        out_specs=(
            P(("dp", "mp"), None),
            P("dp", "section"),
            P("section", "dp", "mp"),
            P("section", "dp", "mp"),
        ),
        check_vma=False,
    )
```

```python
import jax
import jax.numpy as jnp
from jax import lax
from jax.experimental import pallas as pl
from jax.experimental.pallas import tpu as pltpu
from jax.sharding import PartitionSpec as P

MESH = pl.DeviceIdType.MESH
F32 = jnp.float32
BF16 = jnp.bfloat16
GELU = 1.702
LANES = 128
PIECES = 2


def unit_rows(values):
    wide = values.astype(F32)
    length = jnp.sqrt(jnp.sum(wide * wide, axis=1, keepdims=True) + 1.0)
    return (wide / length, length)


def unit_backward(unit, length, grad_unit):
    return (grad_unit - unit * jnp.sum(unit * grad_unit, axis=1, keepdims=True)) / length


def dot_nn(a, b):
    return lax.dot_general(a, b, (((1,), (0,)), ((), ())), preferred_element_type=F32)


def dot_nt(a, b):
    return lax.dot_general(a, b, (((1,), (1,)), ((), ())), preferred_element_type=F32)


def dot_tn(a, b):
    return lax.dot_general(a, b, (((0,), (0,)), ((), ())), preferred_element_type=F32)


def tile(index, size):
    return pl.ds(pl.multiple_of(index * size, size), size)


def make_kernel(n_sec, n_dp, n_mp):
    cores = 2 if n_mp % 2 == 0 else 1
    chips = n_mp // cores

    def kernel(
        text, image, scale_ref, hidden, w_in, w_out,
        image_out, input_out, first_out, second_out,
        text_low, cols, scores, sgrad, row_max, row_lse, row_st, row_rx, col_st, col_rx,
        wi_all, wo_all, t_tx, t_rx, t_own, g_all, g_acc, g_new, act_all, pre_all,
        w_tx, w_rx, i_tx, i_rx,
        gat_s, gat_r, fwd_s, fwd_r, cs_s, cs_r, rs_s, rs_r, wi_s, wi_r, wo_s, wo_r,
        t_s, t_r, g_s, g_r, x_s, x_r, in_s, in_r, ix_s, ix_r, w_s, w_r, im_s, im_r, io_s, io_r,
    ):
        s = lax.axis_index("section")
        d = lax.axis_index("dp")
        m = lax.axis_index("mp")
        last = n_sec - 1
        rows = text.shape[0]
        own = image.shape[0]
        half = own // n_sec
        quarter = rows // n_mp
        step = quarter // PIECES
        feats = text.shape[1]
        share = feats // n_dp
        width = feats // n_sec
        mult = scale_ref[0]
        core = lax.rem(m, cores)
        chip = m // cores

        def copy(src, dst, send, recv, where):
            return pltpu.make_async_remote_copy(
                src_ref=src, dst_ref=dst, send_sem=send, recv_sem=recv,
                device_id=where, device_id_type=MESH,
            )

        def others(mine, count):
            return [lax.rem(mine + k, count) for k in range(1, count)]

        def sources(mine, count):
            return [lax.rem(mine + count - k, count) for k in range(1, count)]

        barrier = pltpu.get_barrier_semaphore()
        for p in others(d, n_dp):
            pl.semaphore_signal(barrier, inc=1, device_id={"dp": p}, device_id_type=MESH)
        for p in others(m, n_mp):
            pl.semaphore_signal(barrier, inc=1, device_id={"mp": p}, device_id_type=MESH)
        for p in others(s, n_sec):
            pl.semaphore_signal(barrier, inc=1, device_id={"section": p}, device_id_type=MESH)

        own_unit, _ = unit_rows(image[...])
        cols[tile(d, own), :] = own_unit.astype(BF16)
        pl.semaphore_wait(barrier, n_dp + n_mp + n_sec - 3)

        def cut(block, sec):
            return cols.at[pl.ds(pl.multiple_of(block * own + sec * half, half), half), :]

        gathers = []
        for p in others(d, n_dp):
            c = copy(cut(d, s), cut(d, s), gat_s.at[p], gat_r.at[d], {"dp": p})
            c.start()
            gathers.append(c)

        class Spread:
            def __init__(self, slot, send, recv):
                self.slot, self.send, self.recv = slot, send, recv
                self.sent = []

            def push(self, index, to):
                c = copy(self.slot(index), self.slot(index), self.send(len(self.sent)),
                         self.recv(index), {"mp": to})
                c.start()
                self.sent.append(c)

            def arrived(self, index):
                copy(self.slot(index), self.slot(index), self.send(0),
                     self.recv(index), {"mp": lax.rem(m + 1, n_mp)}).wait_recv()

            def start(self):
                for q in others(chip, chips):
                    self.push(m, q * cores + core)
                for e in others(core, cores):
                    self.push(m, chip * cores + e)

            def relay(self):
                for q in sources(chip, chips):
                    index = q * cores + core
                    self.arrived(index)
                    for e in others(core, cores):
                        self.push(index, chip * cores + e)

            def finish(self):
                for e in sources(core, cores):
                    self.arrived(chip * cores + e)
                    for q in sources(chip, chips):
                        self.arrived(q * cores + e)

            def drain(self):
                for c in self.sent:
                    c.wait_send()

        wi_all[m] = w_in[...]
        wo_all[m] = w_out[...]
        wi_spread = Spread(lambda k: wi_all.at[k], lambda k: wi_s.at[k], lambda k: wi_r.at[k])
        wo_spread = Spread(lambda k: wo_all.at[k], lambda k: wo_s.at[k], lambda k: wo_r.at[k])
        wi_spread.start()
        wo_spread.start()

        @pl.loop(0, n_mp)
        def _(r):
            unit, _ = unit_rows(text[tile(r, quarter), :])
            text_low[tile(r, quarter), :] = unit.astype(BF16)

        row_max[...] = jnp.full(row_max.shape, -1e30, F32)

        def block_scores(p):
            piece = cols[tile(p, own), :]

            def chunk(r, peak):
                value = mult * dot_nt(text_low[tile(r, quarter), :], piece)
                scores[tile(r, quarter), tile(p, own)] = value
                best = row_max[tile(r, quarter), :]
                for k in range(0, own, LANES):
                    best = jnp.maximum(best, value[:, k : k + LANES])
                row_max[tile(r, quarter), :] = best
                return jnp.maximum(peak, jnp.max(value, axis=0, keepdims=True))

            peak = lax.fori_loop(0, n_mp, chunk, jnp.full((1, own), -1e30, F32))

            def total(r, acc):
                value = scores[tile(r, quarter), tile(p, own)]
                return acc + jnp.sum(jnp.exp(value - peak), axis=0, keepdims=True)

            acc = lax.fori_loop(0, n_mp, total, jnp.zeros((1, own), F32))
            col_st[pl.ds(p, 1), :] = peak
            col_st[pl.ds(n_dp + p, 1), :] = acc

        block_scores(d)
        forwards = []
        for k, p in enumerate(sources(d, n_dp)):
            copy(cut(p, s), cut(p, s), gat_s.at[p], gat_r.at[p], {"dp": p}).wait_recv()
            for t in others(s, n_sec):
                c = copy(cut(p, s), cut(p, s), fwd_s.at[t, p], fwd_r.at[s, p], {"section": t})
                c.start()
                forwards.append(c)
        for p in sources(d, n_dp):
            for t in sources(s, n_sec):
                copy(cut(p, t), cut(p, t), fwd_s.at[t, p], fwd_r.at[t, p],
                     {"section": t}).wait_recv()
            block_scores(p)

        col_rx[d] = col_st[...]
        col_sent = []
        for p in others(d, n_dp):
            c = copy(col_st, col_rx.at[d], cs_s.at[p], cs_r.at[d], {"dp": p})
            c.start()
            col_sent.append(c)

        for r in range(n_mp):
            part = pl.ds(r * quarter, quarter)
            peak = jnp.max(row_max[part, :], axis=1, keepdims=True)

            def total(p, acc):
                value = jnp.exp(scores[part, tile(p, own)] - peak)
                for k in range(0, own, LANES):
                    acc = acc + value[:, k : k + LANES]
                return acc

            acc = lax.fori_loop(0, n_dp, total, jnp.zeros((quarter, LANES), F32))
            acc = jnp.sum(acc, axis=1, keepdims=True)
            wide_peak = jnp.broadcast_to(peak, (quarter, LANES)).T
            wide_sum = jnp.broadcast_to(acc, (quarter, LANES)).T
            row_st[r : r + 1, :] = wide_peak[0:1, :]
            row_st[n_mp + r : n_mp + r + 1, :] = wide_sum[0:1, :]

        row_rx[m] = row_st[...]
        row_sent = []
        for p in others(m, n_mp):
            c = copy(row_st, row_rx.at[m], rs_s.at[p], rs_r.at[m], {"mp": p})
            c.start()
            row_sent.append(c)

        def merge(rx, count, n):
            peak = rx[0, 0:n, :]
            for k in range(1, count):
                peak = jnp.maximum(peak, rx[k, 0:n, :])
            acc = jnp.zeros(peak.shape, F32)
            for k in range(count):
                acc = acc + rx[k, n : 2 * n, :] * jnp.exp(rx[k, 0:n, :] - peak)
            return peak + jnp.log(acc)

        for p in sources(d, n_dp):
            copy(col_st, col_rx.at[p], cs_s.at[p], cs_r.at[p], {"dp": p}).wait_recv()
        col_lse = merge(col_rx, n_dp, n_dp)
        col_st_rows = [col_lse[k : k + 1, :] for k in range(n_dp)]
        for p in sources(m, n_mp):
            copy(row_st, row_rx.at[p], rs_s.at[p], rs_r.at[p], {"mp": p}).wait_recv()
        merged = merge(row_rx, n_mp, n_mp)
        for r in range(n_mp):
            row_lse[r] = jnp.broadcast_to(merged[r : r + 1, :], (LANES, quarter)).T

        def score_rows(r):
            line = row_lse[r]
            text_id = lax.broadcasted_iota(jnp.int32, (quarter, LANES), 0) + d * rows + r * quarter
            for p in range(n_dp):
                for k in range(0, own, LANES):
                    value = scores[tile(r, quarter), p * own + k : p * own + k + LANES]
                    both = jnp.exp(value - line) + jnp.exp(value - col_st_rows[p][:, k : k + LANES])
                    image_id = lax.broadcasted_iota(jnp.int32, (quarter, LANES), 1) + (
                        (p * n_mp + m) * own + k
                    )
                    out = 0.5 * both - jnp.where(text_id == image_id, 1.0, 0.0)
                    sgrad[tile(r, quarter), p * own + k : p * own + k + LANES] = out.astype(BF16)

        @pl.loop(0, n_mp)
        def _(k):
            to_chip = lax.rem(chip + 1 + k // cores, chips)
            r = to_chip * cores + lax.rem(core + 1 + lax.rem(k, cores), cores)
            score_rows(r)

            @pl.when(s == last)
            def _():
                value = dot_nn(sgrad[tile(r, quarter), :], cols[...])

                @pl.when(k < n_mp - 1)
                def _():
                    t_tx[r] = value.astype(BF16)
                    copy(t_tx.at[r], t_rx.at[m], t_s.at[r], t_r.at[m], {"mp": r}).start()

                @pl.when(k == n_mp - 1)
                def _():
                    t_own[...] = value

        def image_part(p):
            at = pl.ds(pl.multiple_of(p * own + s * half, half), half)
            return dot_tn(sgrad[:, at], text_low[...])

        image_sent = []
        for p in others(d, n_dp):
            i_tx[p] = image_part(p).astype(BF16)
            c = copy(i_tx.at[p], i_rx.at[d], im_s.at[p], im_r.at[d], {"dp": p})
            c.start()
            image_sent.append(c)

        wi_spread.relay()
        wo_spread.relay()

        mine = tile(m, quarter)

        @pl.when(s == last)
        def _():
            total = t_own[...]
            for p in sources(m, n_mp):
                copy(t_tx.at[p], t_rx.at[p], t_s.at[p], t_r.at[p], {"mp": p}).wait_recv()
                total = total + t_rx[p].astype(F32)
            unit, length = unit_rows(text[mine, :])
            g_all[m] = unit_backward(unit, length, mult * total).astype(BF16)

        wi_spread.finish()
        wo_spread.finish()

        def slopes(pre, back):
            sigm = 1.0 / (1.0 + jnp.exp(-GELU * pre))
            grad = back * (sigm + GELU * pre * sigm * (1.0 - sigm))
            return (pre * sigm).astype(BF16), grad.astype(BF16)

        def slab(k):
            return input_out.at[tile(k, quarter), :]

        def final(t, piece):
            part = pl.ds(piece * step, step)
            return copy(g_new.at[part, t * width : (t + 1) * width], slab(m).at[part, :],
                        ix_s.at[t, piece], ix_r.at[piece], {"section": t})

        def hop(piece, to):
            part = pl.ds(piece * step, step)
            return copy(g_new.at[part, :], g_all.at[m, part, :], x_s.at[piece], x_r.at[piece],
                        {"section": to})

        g_spreads = []
        for piece in range(PIECES):
            part = pl.ds(piece * step, step)

            @pl.when(s != last)
            def _():
                hop(piece, s + 1).wait_recv()

            spread = Spread(lambda k, part=part: g_all.at[k, part, :],
                            lambda k, piece=piece: g_s.at[piece, k],
                            lambda k, piece=piece: g_r.at[piece, k])
            spread.start()
            g_spreads.append(spread)
            g_acc[part, :] = g_all[m, part, :].astype(F32)
            rows_now = hidden[pl.ds(pl.multiple_of(m * quarter + piece * step, step), step), :]

            @pl.loop(0, n_mp)
            def _(j):
                pre = dot_nn(rows_now, wi_all[j])
                back = dot_nt(g_all[m, part, :], wo_all[j])
                _, grad = slopes(pre, back)
                g_acc[part, :] += dot_nt(grad, wi_all[j])

            g_new[part, :] = g_acc[part, :].astype(BF16)

            @pl.when(s > 0)
            def _():
                hop(piece, s - 1).start()

            @pl.when(s == 0)
            def _():
                for t in range(1, n_sec):
                    final(t, piece).start()

        @pl.when(s == 0)
        def _():
            input_out[mine, :] = g_new[:, 0:width]

        for spread in g_spreads:
            spread.relay()
        in_spread = Spread(slab, lambda k: in_s.at[k], lambda k: in_r.at[k])

        def weight_rows(r):
            pre = dot_nn(hidden[tile(r, quarter), :], w_in[...])
            back = dot_nt(g_all[r], w_out[...])
            act, grad = slopes(pre, back)
            act_all[tile(r, quarter), :] = act
            pre_all[tile(r, quarter), :] = grad

        weight_rows(m)
        for q in sources(chip, chips):
            weight_rows(q * cores + core)
        for e in sources(core, cores):
            for index in [chip * cores + e] + [q * cores + e for q in sources(chip, chips)]:
                for spread in g_spreads:
                    spread.arrived(index)
                weight_rows(index)

        g_rows = g_all[...].reshape(rows, feats)
        grad_second = dot_tn(g_rows, act_all[...])
        for p in range(n_dp):
            w_tx[p, 1] = grad_second[p * share : (p + 1) * share, :].astype(BF16)
        weight_sent = []

        def send_weights(which):
            for p in others(d, n_dp):
                c = copy(w_tx.at[p, which], w_rx.at[d, which], w_s.at[which, p],
                         w_r.at[which, d], {"dp": p})
                c.start()
                weight_sent.append(c)

        send_weights(1)
        grad_first = dot_tn(hidden[...], pre_all[...])
        for p in range(n_dp):
            w_tx[p, 0] = grad_first[p * share : (p + 1) * share, :].astype(BF16)
        send_weights(0)

        @pl.when(s != 0)
        def _():
            for piece in range(PIECES):
                final(0, piece).wait_recv()

        in_spread.start()

        image_half = pl.ds(pl.multiple_of(s * half, half), half)
        total = image_part(d)
        for p in sources(d, n_dp):
            copy(i_tx.at[p], i_rx.at[p], im_s.at[p], im_r.at[p], {"dp": p}).wait_recv()
            total = total + i_rx[p].astype(F32)
        unit, length = unit_rows(image[image_half, :])
        image_out[image_half, :] = unit_backward(unit, length, mult * total).astype(BF16)
        out_sent = []
        for t in others(s, n_sec):
            c = copy(image_out.at[image_half, :], image_out.at[image_half, :],
                     io_s.at[t], io_r.at[s], {"section": t})
            c.start()
            out_sent.append(c)

        in_spread.relay()
        in_spread.finish()

        for which, out in ((1, second_out), (0, first_out)):
            total = w_tx[d, which].astype(F32)
            for p in sources(d, n_dp):
                copy(w_tx.at[p, which], w_rx.at[p, which], w_s.at[which, p],
                     w_r.at[which, p], {"dp": p}).wait_recv()
                total = total + w_rx[p, which].astype(F32)
            out[...] = total

        for t in sources(s, n_sec):
            part = image_out.at[pl.ds(pl.multiple_of(t * half, half), half), :]
            copy(part, part, io_s.at[t], io_r.at[t], {"section": t}).wait_recv()

        for c in gathers + forwards + col_sent + row_sent + image_sent + weight_sent + out_sent:
            c.wait_send()
        for spread in (wi_spread, wo_spread, *g_spreads, in_spread):
            spread.drain()

        @pl.when(s == last)
        def _():
            for p in others(m, n_mp):
                copy(t_tx.at[p], t_rx.at[m], t_s.at[p], t_r.at[m], {"mp": p}).wait_send()

        @pl.when(s > 0)
        def _():
            for piece in range(PIECES):
                hop(piece, s - 1).wait_send()

        @pl.when(s == 0)
        def _():
            for t in range(1, n_sec):
                for piece in range(PIECES):
                    final(t, piece).wait_send()

    return kernel


def solution(mesh):
    n_sec, n_dp, n_mp = mesh.shape["section"], mesh.shape["dp"], mesh.shape["mp"]

    def body(text, image, scale, hidden, w_in, w_out):
        rows, feats = text.shape
        own = image.shape[0]
        hid = w_in.shape[2]
        quarter, half, share = rows // n_mp, own // n_sec, feats // n_dp
        columns = own * n_dp
        dma = pltpu.SemaphoreType.DMA
        vmem = pl.BlockSpec(memory_space=pltpu.VMEM)
        out = pl.pallas_call(
            make_kernel(n_sec, n_dp, n_mp),
            out_shape=(
                jax.ShapeDtypeStruct((own, feats), BF16),
                jax.ShapeDtypeStruct((rows, feats // n_sec), BF16),
                jax.ShapeDtypeStruct((share, hid), F32),
                jax.ShapeDtypeStruct((share, hid), F32),
            ),
            in_specs=[vmem, vmem, pl.BlockSpec(memory_space=pltpu.SMEM), vmem, vmem, vmem],
            out_specs=(vmem,) * 4,
            scratch_shapes=[
                pltpu.VMEM((rows, feats), BF16),
                pltpu.VMEM((columns, feats), BF16),
                pltpu.VMEM((rows, columns), F32),
                pltpu.VMEM((rows, columns), BF16),
                pltpu.VMEM((rows, LANES), F32),
                pltpu.VMEM((n_mp, quarter, LANES), F32),
                pltpu.VMEM((2 * n_mp, quarter), F32),
                pltpu.VMEM((n_mp, 2 * n_mp, quarter), F32),
                pltpu.VMEM((2 * n_dp, own), F32),
                pltpu.VMEM((n_dp, 2 * n_dp, own), F32),
                pltpu.VMEM((n_mp, feats, hid), BF16),
                pltpu.VMEM((n_mp, hid, feats), BF16),
                pltpu.VMEM((n_mp, quarter, feats), BF16),
                pltpu.VMEM((n_mp, quarter, feats), BF16),
                pltpu.VMEM((quarter, feats), F32),
                pltpu.VMEM((n_mp, quarter, feats), BF16),
                pltpu.VMEM((quarter, feats), F32),
                pltpu.VMEM((quarter, feats), BF16),
                pltpu.VMEM((rows, hid), BF16),
                pltpu.VMEM((rows, hid), BF16),
                pltpu.VMEM((n_dp, 2, share, hid), BF16),
                pltpu.VMEM((n_dp, 2, share, hid), BF16),
                pltpu.VMEM((n_dp, half, feats), BF16),
                pltpu.VMEM((n_dp, half, feats), BF16),
                dma((n_dp,)), dma((n_dp,)),
                dma((n_sec, n_dp)), dma((n_sec, n_dp)),
                dma((n_dp,)), dma((n_dp,)),
                dma((n_mp,)), dma((n_mp,)),
                dma((2 * n_mp,)), dma((n_mp,)),
                dma((2 * n_mp,)), dma((n_mp,)),
                dma((n_mp,)), dma((n_mp,)),
                dma((PIECES, 2 * n_mp)), dma((PIECES, n_mp)),
                dma((PIECES,)), dma((PIECES,)),
                dma((2 * n_mp,)), dma((n_mp,)),
                dma((n_sec, PIECES)), dma((PIECES,)),
                dma((2, n_dp)), dma((2, n_dp)),
                dma((n_dp,)), dma((n_dp,)),
                dma((n_sec,)), dma((n_sec,)),
            ],
            compiler_params=pltpu.CompilerParams(
                collective_id=0, has_side_effects=True, vmem_limit_bytes=63000000
            ),
        )(text, image, scale, hidden[0], w_in[0], w_out[0])
        image_grad, input_grad, first, second = out
        return (image_grad, input_grad, first[None], second[None])

    return jax.shard_map(
        body,
        mesh=mesh,
        in_specs=(
            P("dp", None),
            P(("dp", "mp"), None),
            P(),
            P("section", "dp", None),
            P("section", None, "mp"),
            P("section", "mp", None),
        ),
        out_specs=(
            P(("dp", "mp"), None),
            P("dp", "section"),
            P("section", "dp", "mp"),
            P("section", "dp", "mp"),
        ),
        check_vma=False,
    )
```
